32 devices in a mesh: seq: 16 (over z, y, core), fsdp: 2 (over x).
Axes of the slice: x: 2, y: 2, z: 4, core: 2. Of those that a mesh axis runs over, the one named last changes fastest.
Arguments:
- tokens: bfloat16 [8192, 5376], P(('seq', 'fsdp')), may hold values from -6 to 6
- norm_gain: float32 [5376], replicated, may hold values from 0.1 to 1.9
- query_weight: bfloat16 [5376, 2048], P('seq', 'fsdp'), may hold values from -0.078125 to 0.078125
- key_matrix: bfloat16 [5376, 1024], P('seq', 'fsdp'), may hold values from -0.078125 to 0.078125
- value_matrix: bfloat16 [5376, 1024], P('seq', 'fsdp'), may hold values from -0.078125 to 0.078125
- out_weight: bfloat16 [5376, 2048], P('seq', 'fsdp'), may hold values from -0.125 to 0.125
- query_gain: float32 [128], replicated, may hold values from 0.1 to 1.9
- key_gain: float32 [128], replicated, may hold values from 0.1 to 1.9
- post_gain: float32 [5376], replicated, may hold values from 0.1 to 1.9
Outputs:
- layer_out: bfloat16 [8192, 5376], P(('seq', 'fsdp'))
The draws below stay inside these ranges and needn't reach their ends.
All inputs are finite; a program needn't handle non-finite values.
Results may differ from the reference program's by a relative error of at most 0.011.
Values may be sent and summed in bfloat16 or wider, within the bound.
A program may use at most 192 MiB of HBM per device.

```python
import jax
import jax.numpy as jnp
from jax import lax

MODEL_WIDTH = 5376
HEAD_SIZE = 128
QUERY_HEADS = 16
KEY_VALUE_HEADS = 8
WINDOW_LENGTH = 1024
TOKENS = 8192
N_FSDP = 2


def levels(rng, extent, split, least, high):
    level = 1.0
    for dim, shards_of in split:
        steps = jax.random.uniform(jax.random.fold_in(jax.random.fold_in(rng, 6), dim), (shards_of,), jnp.float32, least / len(split), high / len(split))
        level = level * jnp.repeat(jnp.exp(steps), extent[dim] // shards_of).reshape((-1,) + (1,) * (len(extent) - 1 - dim))
    return level


def bell_draw(stream_key, dims, scale, most, pieces=(), kind=jnp.bfloat16):
    loudness = levels(stream_key, dims, pieces, -0.22, 0.18) if pieces else 1.0
    drawn = jax.random.normal(stream_key, dims, jnp.float32) * scale * loudness
    return jnp.minimum(jnp.maximum(drawn, -most), most).astype(kind)


def setup_inputs(seed: int = 0) -> dict:
    key_of = jax.random.split(jax.random.key(seed), 10)
    return {
        "tokens": bell_draw(key_of[0], (TOKENS, MODEL_WIDTH), 1.0, 6.0, ((0, 32),)),
        "norm_gain": jnp.clip(1.0 + 0.18 * jax.random.normal(key_of[1], (MODEL_WIDTH,), jnp.float32), 0.1, 1.9),
        "query_weight": bell_draw(key_of[2], (MODEL_WIDTH, QUERY_HEADS * HEAD_SIZE), MODEL_WIDTH ** -0.5, 0.078125, ((0, 16), (1, 2))),
        "key_matrix": bell_draw(key_of[3], (MODEL_WIDTH, KEY_VALUE_HEADS * HEAD_SIZE), MODEL_WIDTH ** -0.5, 0.078125, ((0, 16), (1, 2))),
        "value_matrix": bell_draw(key_of[4], (MODEL_WIDTH, KEY_VALUE_HEADS * HEAD_SIZE), MODEL_WIDTH ** -0.5, 0.078125, ((0, 16), (1, 2))),
        "out_weight": bell_draw(key_of[5], (MODEL_WIDTH, QUERY_HEADS * HEAD_SIZE), (QUERY_HEADS * HEAD_SIZE) ** -0.5, 0.125, ((0, 16), (1, 2))),
        "query_gain": jnp.clip(1.0 + 0.18 * jax.random.normal(key_of[6], (HEAD_SIZE,), jnp.float32), 0.1, 1.9),
        "key_gain": jnp.clip(1.0 + 0.18 * jax.random.normal(key_of[7], (HEAD_SIZE,), jnp.float32), 0.1, 1.9),
        "post_gain": jnp.clip(1.0 + 0.18 * jax.random.normal(key_of[8], (MODEL_WIDTH,), jnp.float32), 0.1, 1.9),
    }


epsilon = 1e-06
score_scale = 168.0 ** (-0.5)
rope_base = 10000.0
masked_score = -1e+30

def rms_scaled(values, gain):
    mean_square = lax.optimization_barrier(jnp.mean(values * values, axis=-1, keepdims=True))
    return values * lax.rsqrt(mean_square + epsilon) * gain

def rotary(values, positions):
    half_width = values.shape[-1] // 2
    exponents = jnp.arange(half_width, dtype=jnp.float32) * (2.0 / values.shape[-1])
    frequency = jnp.exp(-exponents * jnp.log(jnp.float32(rope_base)))
    angles = positions.astype(jnp.float32)[:, None] * frequency[None, :]
    cosine = jnp.cos(angles)[:, None, :]
    sine = jnp.sin(angles)[:, None, :]
    first_half = values[..., :half_width]
    second_half = values[..., half_width:]
    return jnp.concatenate([first_half * cosine - second_half * sine, second_half * cosine + first_half * sine], axis=-1)

def head_states(projected, gain, positions):
    shaped = projected.reshape(projected.shape[0], -1, HEAD_SIZE)
    return rotary(rms_scaled(shaped, gain), positions).astype(jnp.bfloat16)

def window_block(query_block, key_block, value_block, query_pos, key_pos):
    scores = jnp.einsum('rkgd,lkd->kgrl', query_block.astype(jnp.float32), key_block.astype(jnp.float32), precision=lax.Precision.HIGHEST) * score_scale
    offset = query_pos[:, None] - key_pos[None, :]
    allowed = (offset >= 0) & (offset < WINDOW_LENGTH) & (key_pos[None, :] >= 0)
    scores = jnp.where(allowed, scores, masked_score)
    highest = lax.optimization_barrier(jnp.max(scores, axis=-1, keepdims=True))
    raised = jnp.exp(scores - highest)
    weights = (raised / lax.optimization_barrier(jnp.sum(raised, axis=-1, keepdims=True))).astype(jnp.bfloat16)
    mixed = jnp.einsum('kgrl,lkd->rkgd', weights.astype(jnp.float32), value_block.astype(jnp.float32), precision=lax.Precision.HIGHEST)
    return mixed.astype(jnp.bfloat16).reshape(query_block.shape[0], -1)

def reference(tokens, norm_gain, query_weight, key_matrix, value_matrix, out_weight, query_gain, key_gain, post_gain):
    row_count = tokens.shape[0]
    query_groups = QUERY_HEADS // KEY_VALUE_HEADS
    normed_input = rms_scaled(tokens.astype(jnp.float32), norm_gain).astype(jnp.bfloat16)
    positions = jnp.arange(row_count, dtype=jnp.int32)
    query_states = head_states(jnp.dot(normed_input, query_weight, preferred_element_type=jnp.float32), query_gain, positions)
    query_states = query_states.reshape(row_count, KEY_VALUE_HEADS, query_groups, HEAD_SIZE)
    keys_all = head_states(jnp.dot(normed_input, key_matrix, preferred_element_type=jnp.float32), key_gain, positions)
    value_states = jnp.dot(normed_input, value_matrix, preferred_element_type=jnp.float32).astype(jnp.bfloat16).reshape(row_count, KEY_VALUE_HEADS, HEAD_SIZE)
    padding_rows = jnp.zeros((WINDOW_LENGTH, KEY_VALUE_HEADS, HEAD_SIZE), jnp.bfloat16)
    padded_keys = jnp.concatenate([padding_rows, keys_all], axis=0)
    padded_values = jnp.concatenate([padding_rows, value_states], axis=0)

    def one_block(block_index):
        begin = (block_index * WINDOW_LENGTH).astype(jnp.int32)
        query_block = lax.dynamic_slice_in_dim(query_states, begin, WINDOW_LENGTH, 0)
        key_block = lax.dynamic_slice_in_dim(padded_keys, begin, 2 * WINDOW_LENGTH, 0)
        value_block = lax.dynamic_slice_in_dim(padded_values, begin, 2 * WINDOW_LENGTH, 0)
        query_pos = begin + jnp.arange(WINDOW_LENGTH, dtype=jnp.int32)
        key_pos = begin - WINDOW_LENGTH + jnp.arange(2 * WINDOW_LENGTH, dtype=jnp.int32)
        return window_block(query_block, key_block, value_block, query_pos, key_pos)
    blocks = lax.map(one_block, jnp.arange(row_count // WINDOW_LENGTH, dtype=jnp.int32))
    attended = blocks.reshape(row_count, QUERY_HEADS * HEAD_SIZE)
    group_width = QUERY_HEADS * HEAD_SIZE // N_FSDP
    projected = jnp.zeros((row_count, out_weight.shape[0]), jnp.float32)
    for group in range(N_FSDP):
        left = attended[:, group * group_width:(group + 1) * group_width]
        right = out_weight[:, group * group_width:(group + 1) * group_width]
        term = lax.dot_general(left, right, (((1,), (1,)), ((), ())), preferred_element_type=jnp.float32)
        projected = projected + term.astype(jnp.bfloat16).astype(jnp.float32)
    return (tokens.astype(jnp.float32) + rms_scaled(projected, post_gain)).astype(jnp.bfloat16)
```

```python
import functools

import jax
import jax.numpy as jnp
from jax import lax
from jax.experimental import pallas as pl
from jax.experimental.pallas import tpu as pltpu
from jax.sharding import PartitionSpec as P

HEAD_SIZE = 128
WINDOW_LENGTH = 1024


epsilon = 1e-06
score_scale = 168.0 ** (-0.5)
rope_base = 10000.0
masked_score = -1e30


def passed_along(block, axis, distance):
    devices = range(lax.axis_size(axis))
    route = [(i - distance, i) for i in devices if i - distance in devices]
    return lax.ppermute(block, axis, route)


def rms_scaled(values, gain):
    mean_square = jnp.mean(values * values, axis=-1, keepdims=True)
    return values * lax.rsqrt(mean_square + epsilon) * gain


def rotary(values, positions):
    half_width = values.shape[-1] // 2
    exponents = jnp.arange(half_width, dtype=jnp.float32) * (2.0 / values.shape[-1])
    frequency = jnp.exp(-exponents * jnp.log(jnp.float32(rope_base)))
    angles = positions.astype(jnp.float32)[:, None] * frequency[None, :]
    cosine = jnp.cos(angles)[:, None, :]
    sine = jnp.sin(angles)[:, None, :]
    first_half = values[..., :half_width]
    second_half = values[..., half_width:]
    return jnp.concatenate(
        [first_half * cosine - second_half * sine, second_half * cosine + first_half * sine],
        axis=-1,
    )


def head_states(projected, gain, positions):
    shaped = projected.reshape(projected.shape[0], -1, HEAD_SIZE)
    return rotary(rms_scaled(shaped, gain), positions).astype(jnp.bfloat16)


def window_block(query_block, key_block, value_block, query_pos, key_pos):
    scores = (
        jnp.einsum("rkgd,lkd->kgrl", query_block, key_block, preferred_element_type=jnp.float32)
        * score_scale
    )
    offset = query_pos[:, None] - key_pos[None, :]
    allowed = (offset >= 0) & (offset < WINDOW_LENGTH) & (key_pos[None, :] >= 0)
    scores = jnp.where(allowed, scores, masked_score)
    highest = jnp.max(scores, axis=-1, keepdims=True)
    raised = jnp.exp(scores - highest)
    weights = (raised / jnp.sum(raised, axis=-1, keepdims=True)).astype(jnp.bfloat16)
    mixed = jnp.einsum("kgrl,lkd->rkgd", weights, value_block, preferred_element_type=jnp.float32)
    return mixed.astype(jnp.bfloat16).reshape(query_block.shape[0], -1)


def ring_place(chip, chips):
    row, side = chip // 2, chip % 2
    return side * (chips - 1 - row) + (1 - side) * row


def ring_chip(place, chips):
    back = place // (chips // 2)
    return back * (2 * (chips - 1 - place) + 1) + (1 - back) * 2 * place


def gather_kernel(
    shards,
    copies,
    query_ref,
    key_ref,
    value_ref,
    tokens_ref,
    query_out,
    key_out,
    value_out,
    tokens_out,
    local_sem,
    ring_send,
    ring_recv,
    pair_send,
    pair_recv,
    token_send,
    token_recv,
):
    chips = shards // 2
    me = lax.axis_index("seq")
    group = lax.axis_index("fsdp")
    core = me % 2
    place = ring_place(me // 2, chips)
    half = query_ref.shape[1] // 2
    other = (me // 2) * 2 + 1 - core
    ahead = ring_chip((place + 1) % chips, chips) * 2 + core
    behind = ring_chip((place + chips - 1) % chips, chips) * 2 + core

    barrier = pltpu.get_barrier_semaphore()
    for device in (other, ahead, behind):
        pl.semaphore_signal(
            barrier, inc=1, device_id=(device, group), device_id_type=pl.DeviceIdType.MESH
        )
    for offset in range(1, copies):
        pl.semaphore_signal(
            barrier,
            inc=1,
            device_id=(me, (group + offset) % copies),
            device_id_type=pl.DeviceIdType.MESH,
        )
    pl.semaphore_wait(barrier, 3 + copies - 1)

    flows = (
        (query_ref, query_out, 0, half, 1),
        (key_ref, key_out, 0, key_ref.shape[1], -1),
        (query_ref, query_out, half, half, 1),
        (value_ref, value_out, 0, value_ref.shape[1], -1),
    )
    pending = []
    arriving = []
    token_slot = tokens_out.at[group]
    ring_copies = {}
    for step in range(chips):
        for index, (source, target, column, width, way) in enumerate(flows):
            columns = pl.ds(column, width)
            owner = ring_chip((place - way * step + chips) % chips, chips) * 2 + core
            slot = target.at[owner, :, columns]
            if step == 0:
                block = source.at[:, columns]
            else:
                block = slot
                ring_copies[index, step - 1].wait_recv()
            if step < chips - 1:
                copy = pltpu.make_async_remote_copy(
                    src_ref=block,
                    dst_ref=slot,
                    send_sem=ring_send.at[index, step],
                    recv_sem=ring_recv.at[index, step],
                    device_id=(ahead if way > 0 else behind, group),
                    device_id_type=pl.DeviceIdType.MESH,
                )
                copy.start()
                ring_copies[index, step] = copy
                pending.append(copy)
            across = pltpu.make_async_remote_copy(
                src_ref=block,
                dst_ref=slot,
                send_sem=pair_send.at[index, step],
                recv_sem=pair_recv.at[index, step],
                device_id=(other, group),
                device_id_type=pl.DeviceIdType.MESH,
            )
            across.start()
            pending.append(across)
            arriving.append(across)
        if step == 0:
            for offset in range(1, copies):
                swap = pltpu.make_async_remote_copy(
                    src_ref=tokens_ref,
                    dst_ref=token_slot,
                    send_sem=token_send.at[offset - 1],
                    recv_sem=token_recv.at[offset - 1],
                    device_id=(me, (group + offset) % copies),
                    device_id_type=pl.DeviceIdType.MESH,
                )
                swap.start()
                pending.append(swap)
                arriving.append(swap)
            local = [
                pltpu.make_async_copy(query_ref, query_out.at[me], local_sem.at[0]),
                pltpu.make_async_copy(key_ref, key_out.at[me], local_sem.at[1]),
                pltpu.make_async_copy(value_ref, value_out.at[me], local_sem.at[2]),
                pltpu.make_async_copy(tokens_ref, token_slot, local_sem.at[3]),
            ]
            for copy in local:
                copy.start()
    for copy in arriving:
        copy.wait_recv()
    for copy in pending:
        copy.wait_send()
    for copy in local:
        copy.wait()


def gathered(query_weight, key_matrix, value_matrix, tokens):
    shards, copies = lax.axis_size("seq"), lax.axis_size("fsdp")
    inputs = (query_weight, key_matrix, value_matrix, tokens)
    counts = (shards, shards, shards, copies)
    outputs = [
        jax.ShapeDtypeStruct((n, *a.shape), a.dtype) for a, n in zip(inputs, counts)
    ]
    chips = shards // 2
    anywhere = pl.BlockSpec(memory_space=pltpu.MemorySpace.HBM)
    whole = pl.pallas_call(
        functools.partial(gather_kernel, shards, copies),
        out_shape=outputs,
        in_specs=[anywhere] * 4,
        out_specs=[anywhere] * 4,
        scratch_shapes=[
            pltpu.SemaphoreType.DMA((4,)),
            pltpu.SemaphoreType.DMA((4, chips)),
            pltpu.SemaphoreType.DMA((4, chips)),
            pltpu.SemaphoreType.DMA((4, chips)),
            pltpu.SemaphoreType.DMA((4, chips)),
            pltpu.SemaphoreType.DMA((copies,)),
            pltpu.SemaphoreType.DMA((copies,)),
        ],
        compiler_params=pltpu.CompilerParams(collective_id=0, has_side_effects=True),
    )(*inputs)
    return [a.reshape(-1, a.shape[-1]) for a in whole]


def on_device(
    tokens,
    norm_gain,
    query_weight,
    key_matrix,
    value_matrix,
    out_weight,
    query_gain,
    key_gain,
    post_gain,
):
    query_full, key_full, value_full, pair_rows = gathered(
        query_weight, key_matrix, value_matrix, tokens
    )
    out_weight, pair_rows = lax.optimization_barrier((out_weight, pair_rows))
    out_full = lax.all_gather(out_weight, "seq", axis=0, tiled=True)
    shard_rows = pair_rows.shape[0]
    first_row = lax.axis_index("seq") * shard_rows
    normed_input = rms_scaled(pair_rows.astype(jnp.float32), norm_gain).astype(jnp.bfloat16)
    query_width = query_weight.shape[1]
    key_width = key_matrix.shape[1]
    local_heads = key_width // HEAD_SIZE
    query_groups = query_width // key_width
    keys_raw = jnp.dot(normed_input, key_full, preferred_element_type=jnp.float32)
    values_raw = jnp.dot(normed_input, value_full, preferred_element_type=jnp.float32)
    queries_raw = jnp.dot(normed_input, query_full, preferred_element_type=jnp.float32)
    positions = first_row + jnp.arange(shard_rows, dtype=jnp.int32)
    query_states = head_states(queries_raw, query_gain, positions).reshape(
        shard_rows, local_heads, query_groups, HEAD_SIZE
    )
    keys_now = head_states(keys_raw, key_gain, positions).reshape(shard_rows, key_width)
    values_now = values_raw.astype(jnp.bfloat16)
    stacked = jnp.stack([keys_now, values_now])
    reach = min(WINDOW_LENGTH, shard_rows)
    count = WINDOW_LENGTH // reach
    received = []
    for distance in range(1, count + 1):
        received = [passed_along(stacked, "seq", distance)] + received
    window_rows = jnp.concatenate(received + [stacked], axis=1)
    copies = lax.axis_size("fsdp")
    group = lax.axis_index("fsdp")
    part_rows = shard_rows // copies
    part_keys = window_rows.shape[1] - shard_rows + part_rows

    def partial_rows(part, states):
        begin = part * part_rows
        queries = lax.dynamic_slice_in_dim(states, begin, part_rows, 0)
        window = lax.dynamic_slice_in_dim(window_rows, begin, part_keys, 1)
        keys = window[0].reshape(part_keys, local_heads, HEAD_SIZE)
        values = window[1].reshape(part_keys, local_heads, HEAD_SIZE)
        query_pos = first_row + begin + jnp.arange(part_rows, dtype=jnp.int32)
        key_pos = first_row + begin - WINDOW_LENGTH + jnp.arange(part_keys, dtype=jnp.int32)
        attended = window_block(queries, keys, values, query_pos, key_pos)
        return lax.dot_general(
            attended, out_full, (((1,), (1,)), ((), ())), preferred_element_type=jnp.float32
        ).astype(jnp.bfloat16)

    summed = 0.0
    for offset in range(1, copies):
        away = partial_rows((group + offset) % copies, query_states)
        route = [(i, (i + offset) % copies) for i in range(copies)]
        query_states, away = lax.optimization_barrier((query_states, away))
        summed = summed + lax.ppermute(away, "fsdp", route).astype(jnp.float32)
    summed = partial_rows(group, query_states).astype(jnp.float32) + summed
    return (tokens.astype(jnp.float32) + rms_scaled(summed, post_gain)).astype(jnp.bfloat16)


def solution(mesh):
    in_specs = (
        P(("seq", "fsdp"), None),
        P(),
        P("seq", "fsdp"),
        P("seq", "fsdp"),
        P("seq", "fsdp"),
        P("seq", "fsdp"),
        P(),
        P(),
        P(),
    )
    out_specs = P(("seq", "fsdp"), None)
    return jax.shard_map(
        on_device, mesh=mesh, in_specs=in_specs, out_specs=out_specs, check_vma=False
    )
```
